32 devices in a mesh: blk: 32 (over z, y, x, core).
Axes of the slice: x: 2, y: 2, z: 4, core: 2. Of those that a mesh axis runs over, the one named last changes fastest.
Arguments:
- x_points: bfloat16 [1024, 128], P('blk'), may hold values from -5.2 to 5.2, as said below
- y_points: bfloat16 [1024, 128], P('blk'), may hold values from -5.2 to 5.2, as said below
Outputs:
- x_scores: float32 [1024, 3], P('blk')
- y_scores: float32 [1024, 3], P('blk')
- mmd_stat: float32 [3], replicated
- hsic_stat: float32 [3], replicated
The draws below stay inside these ranges and needn't reach their ends.
Inputs may be any that keep to these rules, and one draw needn't show every extreme that they name: `x_points`: every entry of the first sample lies within -5.2 and 5.2. `y_points`: every entry of the second sample lies within -5.2 and 5.2.
All inputs are finite; a program needn't handle non-finite values.
Results may differ from the reference program's by a relative error of at most 0.00035.
Values may be sent and summed in bfloat16 or wider, within the bound.
A program may use at most 64 MiB of HBM per device.

```python
import jax
import jax.numpy as jnp
from jax import lax

D = 128
PTS_DEV = 32
POINTS = 1024
N_BLK = 32


def clustered(key, member):
    labels = jax.random.randint(jax.random.fold_in(key, 7), (POINTS,), 0, POINTS // 4)
    centres = jnp.clip(jax.random.normal(jax.random.fold_in(key, 20 + member), (POINTS // 4, D), jnp.float32), -4.0, 4.0)
    noise_key = jax.random.fold_in(key, 40 + member)
    spread = jnp.clip(jax.random.normal(noise_key, (POINTS, D), jnp.float32), -4.0, 4.0)
    return (centres[labels] + 0.3 * spread).astype(jnp.bfloat16)


def draw_x_points(key, part):
    return clustered(key, 0)


def draw_y_points(key, part):
    return clustered(key, 1)


def setup_inputs(seed: int = 0) -> dict:
    keys = jax.random.split(jax.random.key(seed), 3)
    return {
        "x_points": draw_x_points(jax.random.fold_in(keys[2], 71), 0),
        "y_points": draw_y_points(jax.random.fold_in(keys[2], 71), 0),
    }


WIDTHS = (0.08, 0.16, 0.32)


def kernels(left, right):
    products = jnp.dot(left, right.T, preferred_element_type=jnp.float32)
    left_sq = jnp.sum(jnp.square(left.astype(jnp.float32)), axis=1)
    right_sq = jnp.sum(jnp.square(right.astype(jnp.float32)), axis=1)
    distance = jnp.maximum(left_sq[:, None] + right_sq[None, :] - 2.0 * products, 0.0)
    factor = 1.0 / (2.0 * jnp.array(WIDTHS, jnp.float32) * left.shape[1])
    return jnp.exp(-factor[:, None, None] * distance[None])


def reference(x_points, y_points):
    def block_rows(offset):
        left_x = lax.dynamic_slice_in_dim(x_points, offset, PTS_DEV, 0)
        left_y = lax.dynamic_slice_in_dim(y_points, offset, PTS_DEV, 0)
        row_index = offset + jnp.arange(PTS_DEV, dtype=jnp.int32)
        col_index = jnp.arange(POINTS, dtype=jnp.int32)
        offdiag = (row_index[:, None] != col_index[None, :]).astype(jnp.float32)
        raw_x = kernels(left_x, x_points)
        raw_y = kernels(left_y, y_points)
        cross_xy = kernels(left_x, y_points)
        cross_yx = kernels(left_y, x_points)
        hadamard = raw_x * raw_y
        return jnp.stack([jnp.sum(raw_x * offdiag, 2), jnp.sum(raw_y * offdiag, 2), jnp.sum(cross_xy, 2), jnp.sum(cross_yx, 2), jnp.sum(hadamard, 2)])

    offsets = jnp.arange(N_BLK, dtype=jnp.int32) * PTS_DEV
    blocks = lax.map(block_rows, offsets)
    sums = jnp.transpose(blocks, (1, 2, 0, 3)).reshape(5, 3, POINTS)
    sum_xx, sum_yy, sum_xy, sum_yx, sum_h = sums[0], sums[1], sums[2], sums[3], sums[4]
    full_x = sum_xx + 1.0
    full_y = sum_yy + 1.0
    count_all = jnp.float32(POINTS)
    mmd_stat = count_all * ((jnp.sum(sum_xx, 1) + jnp.sum(sum_yy, 1)) / (count_all * (count_all - 1.0)) - 2.0 * jnp.sum(sum_xy, 1) / (count_all * count_all))
    hsic_stat = (jnp.sum(sum_h, 1) - 2.0 * jnp.sum(full_x * full_y, 1) / count_all + jnp.sum(full_x, 1) * jnp.sum(full_y, 1) / (count_all * count_all)) / count_all
    x_scores = (jnp.log(sum_xx) - jnp.log(sum_xy)).T
    y_scores = (jnp.log(sum_yy) - jnp.log(sum_yx)).T
    return x_scores, y_scores, mmd_stat, hsic_stat
```

```python
import functools
import math

import jax
import jax.numpy as jnp
from jax import lax
from jax.experimental import pallas as pl
from jax.experimental.pallas import tpu as pltpu
from jax.sharding import PartitionSpec as P

WIDTHS = (0.08, 0.16, 0.32)
LANES = 128
STEP = 16
MESH = pl.DeviceIdType.MESH


def plane_size(count):
    size = math.isqrt(count)
    while size * size < count or count % size:
        size += 1
    return size


def lane_norms(points):
    squares = jnp.square(points.astype(jnp.float32))
    high = squares.astype(jnp.bfloat16)
    low = (squares - high.astype(jnp.float32)).astype(jnp.bfloat16)
    ones = jnp.ones((8, points.shape[1]), jnp.bfloat16)
    dims = (((1,), (1,)), ((), ()))
    return lax.dot_general(
        ones, high, dims, preferred_element_type=jnp.float32
    ) + lax.dot_general(ones, low, dims, preferred_element_type=jnp.float32)


def fold8(array):
    return jnp.sum(array.reshape(array.shape[0] // 8, 8, array.shape[1]), 0)


def powers(widest):
    middle = widest * widest
    return [middle * middle, middle, widest]


def kernel(
    plane,
    depth,
    x_hbm,
    y_hbm,
    x_out,
    y_out,
    mmd_out,
    hsic_out,
    rows,
    cols,
    parts,
    tots,
    turn,
    load_sem,
    row_send,
    row_recv,
    col_send,
    col_recv,
    part_send,
    part_recv,
    tot_send,
    tot_recv,
):
    length, dim = x_hbm.shape
    count = plane * depth * length
    tiles = plane * length // LANES
    chunks = depth * length // LANES
    per_tile = LANES // length
    me = lax.axis_index("blk")
    mine = lax.rem(me, plane)
    layer = me // plane

    loads = [
        pltpu.make_async_copy(source, buffer.at[slot, pl.ds(first, length)], load_sem.at[k])
        for k, (source, buffer, slot, first) in enumerate(
            [
                (x_hbm, rows, mine, 0),
                (y_hbm, rows, mine, length),
                (x_hbm, cols, layer, 0),
                (y_hbm, cols, layer, length),
            ]
        )
    ]
    for load in loads:
        load.start()

    plane_peers = [layer * plane + lax.rem(mine + k, plane) for k in range(1, plane)]
    depth_peers = [lax.rem(layer + k, depth) * plane + mine for k in range(1, depth)]

    barrier = pltpu.get_barrier_semaphore()
    for peer in depth_peers + plane_peers:
        pl.semaphore_signal(barrier, inc=1, device_id=(peer,), device_id_type=MESH)
    for load in loads:
        load.wait()
    pl.semaphore_wait(barrier, plane + depth - 2)

    def spread(buffer, slot, peers, send, recv):
        copies = []
        for k, peer in enumerate(peers):
            copy = pltpu.make_async_remote_copy(
                src_ref=buffer.at[slot],
                dst_ref=buffer.at[slot],
                send_sem=send.at[k],
                recv_sem=recv.at[k],
                device_id=(peer,),
                device_id_type=MESH,
            )
            copy.start()
            copies.append(copy)
        return copies

    col_copies = spread(cols, layer, depth_peers, col_send, col_recv)
    row_copies = spread(rows, mine, plane_peers, row_send, row_recv)
    for copy in row_copies:
        copy.wait_recv()
    for copy in col_copies:
        copy.wait_recv()

    scale = -math.log2(math.e) / (2.0 * WIDTHS[2] * dim)
    dims = (((1,), (1,)), ((), ()))

    def tile_sums(tile):
        blocks = pl.ds(tile * per_tile, per_tile)
        left_x = rows[blocks, :length].reshape(LANES, dim)
        left_y = rows[blocks, length:].reshape(LANES, dim)
        left = jnp.concatenate([left_x, left_y], 0)
        norms = lane_norms(left)
        left_sq_x, left_sq_y = norms[:1, :LANES], norms[:1, LANES:]
        row_index = (
            layer * (plane * length)
            + tile * LANES
            + lax.broadcasted_iota(jnp.int32, (STEP, LANES), 1)
        )

        def chunk_sums(chunk, sums):
            blocks = pl.ds(chunk * per_tile, per_tile)
            right_x = cols[blocks, :length].reshape(LANES, dim)
            right_y = cols[blocks, length:].reshape(LANES, dim)
            right = jnp.concatenate([right_x, right_y], 0)
            right_sq = jnp.sum(jnp.square(right.astype(jnp.float32)), 1, keepdims=True)
            products = lax.dot_general(
                right * jnp.bfloat16(-2.0), left, dims, preferred_element_type=jnp.float32
            )
            sums = list(sums)
            for first in range(0, LANES, STEP):
                inner = lax.broadcasted_iota(jnp.int32, (STEP, LANES), 0)
                col_index = (
                    (chunk * per_tile + first // length) * plane + mine
                ) * length + (inner + first % length)
                diagonal = row_index == col_index
                sq_x = right_sq[first : first + STEP]
                sq_y = right_sq[LANES + first : LANES + first + STEP]

                def widest(left_sq, right_sq, products):
                    distance = jnp.maximum(left_sq + right_sq + products, 0.0)
                    return jnp.exp2(distance * scale)

                top = products[first : first + STEP]
                bottom = products[LANES + first : LANES + first + STEP]
                same_x = widest(left_sq_x, sq_x, top[:, :LANES])
                same_y = widest(left_sq_y, sq_y, bottom[:, LANES:])
                cross_xy = widest(left_sq_x, sq_y, bottom[:, :LANES])
                cross_yx = widest(left_sq_y, sq_x, top[:, LANES:])
                hadamard = same_x * same_y
                same_x = jnp.where(diagonal, 0.0, same_x)
                same_y = jnp.where(diagonal, 0.0, same_y)
                terms = []
                for value in (same_x, same_y, hadamard, cross_xy, cross_yx):
                    terms += powers(value)
                sums = [a + fold8(b) for a, b in zip(sums, terms)]
            return tuple(sums)

        sums = tuple(jnp.zeros((8, LANES), jnp.float32) for _ in range(15))
        if chunks == 1:
            sums = chunk_sums(0, sums)
        else:
            sums = lax.fori_loop(0, chunks, chunk_sums, sums)
        order = [0, 1, 2, 3, 4, 5, 6, 7, 9, 10, 11, 12, 13, 14, 8]
        flat = [jnp.sum(sums[k], 0, keepdims=True) for k in order]
        flat.append(jnp.zeros((1, LANES), jnp.float32))
        parts[mine, tile] = jnp.concatenate(flat, 0)

    if tiles <= 2:
        for tile in range(tiles):
            tile_sums(tile)
    else:

        @pl.loop(0, tiles)
        def _(tile):
            tile_sums(tile)

    part_copies = spread(parts, mine, plane_peers, part_send, part_recv)
    for copy in part_copies:
        copy.wait_recv()

    def whole_sums(tile):
        total = parts[0, tile]
        for k in range(1, plane):
            total = total + parts[k, tile]
        return total[:8], total[8:]

    upper_total = jnp.zeros((8, LANES), jnp.float32)
    lower_total = jnp.zeros((8, LANES), jnp.float32)
    cross_total = jnp.zeros((8, LANES), jnp.float32)
    for tile in range(tiles):
        upper, lower = whole_sums(tile)
        upper_total += upper
        lower_total += lower
        cross_total += (upper + 1.0) * (pltpu.roll(upper, 5, 0) + 1.0)
    lane = lax.broadcasted_iota(jnp.int32, (8, LANES), 1)
    packed = jnp.where(
        lane == 0,
        jnp.sum(upper_total, 1, keepdims=True),
        jnp.where(
            lane == 1,
            jnp.sum(lower_total, 1, keepdims=True),
            jnp.sum(cross_total, 1, keepdims=True),
        ),
    )
    tots[layer] = packed
    tot_copies = spread(tots, layer, depth_peers, tot_send, tot_recv)

    upper, lower = whole_sums(mine // per_tile)
    scores = jnp.log(upper) - jnp.log(lower)
    turn[...] = jnp.concatenate([scores, jnp.zeros((LANES - 8, LANES), jnp.float32)], 0).T
    own = turn[pl.ds(pl.multiple_of(lax.rem(mine, per_tile) * length, length), length)]
    x_out[...] = own[:, :3]
    y_out[...] = pltpu.roll(own, LANES - 3, 1)[:, :3]

    for copy in tot_copies:
        copy.wait_recv()
    total = tots[0]
    for k in range(1, depth):
        total = total + tots[k]
    flat = jnp.concatenate([total, jnp.zeros((LANES - 8, LANES), jnp.float32)], 0).T
    upper, lower, cross = flat[0:1], flat[1:2], flat[2:3]
    paired = pltpu.roll(upper, LANES - 3, 1)
    narrow = pltpu.roll(upper, LANES - 6, 1)
    wide = pltpu.roll(lower, LANES - 4, 1)
    hadamard = jnp.where(lane[:1] < 2, narrow, wide)
    size = float(count)
    rows_all = jnp.float32(size)
    mmd = size * ((upper + paired) / (size * (size - 1.0)) - 2.0 * lower / (size * size))
    hsic = (
        hadamard
        - 2.0 * cross / size
        + (upper + rows_all) * (paired + rows_all) / (size * size)
    ) / size
    mmd_out[...] = mmd[:, :3]
    hsic_out[...] = hsic[:, :3]
    for copy in col_copies + row_copies + part_copies + tot_copies:
        copy.wait_send()


def shards(x_points, y_points):
    length, dim = x_points.shape
    count = lax.axis_size("blk")
    plane = plane_size(count)
    depth = count // plane
    tiles = plane * length // LANES
    dma = pltpu.SemaphoreType.DMA
    x_scores, y_scores, mmd, hsic = pl.pallas_call(
        functools.partial(kernel, plane, depth),
        out_shape=(
            jax.ShapeDtypeStruct((length, 3), jnp.float32),
            jax.ShapeDtypeStruct((length, 3), jnp.float32),
            jax.ShapeDtypeStruct((1, 3), jnp.float32),
            jax.ShapeDtypeStruct((1, 3), jnp.float32),
        ),
        in_specs=[pl.BlockSpec(memory_space=pl.ANY)] * 2,
        out_specs=(pl.BlockSpec(memory_space=pltpu.VMEM),) * 4,
        scratch_shapes=[
            pltpu.VMEM((plane, 2 * length, dim), jnp.bfloat16),
            pltpu.VMEM((depth, 2 * length, dim), jnp.bfloat16),
            pltpu.VMEM((plane, tiles, 16, LANES), jnp.float32),
            pltpu.VMEM((depth, 8, LANES), jnp.float32),
            pltpu.VMEM((LANES, LANES), jnp.float32),
            dma((4,)),
            dma((plane,)),
            dma((plane,)),
            dma((depth,)),
            dma((depth,)),
            dma((plane,)),
            dma((plane,)),
            dma((depth,)),
            dma((depth,)),
        ],
        compiler_params=pltpu.CompilerParams(collective_id=0, has_side_effects=True),
    )(x_points, y_points)
    return x_scores, y_scores, mmd[0], hsic[0]


def solution(mesh):
    placed = (P("blk", None), P("blk", None))
    return jax.shard_map(
        shards,
        mesh=mesh,
        in_specs=placed,
        out_specs=(P("blk", None), P("blk", None), P(), P()),
        check_vma=False,
    )
```

```python
import functools
import math

import jax
import jax.numpy as jnp
from jax import lax
from jax.experimental import pallas as pl
from jax.experimental.pallas import tpu as pltpu
from jax.sharding import PartitionSpec as P

WIDTHS = (0.08, 0.16, 0.32)
LANES = 128
STEP = 16
MESH = pl.DeviceIdType.MESH


def plane_size(count):
    size = math.isqrt(count)
    while size * size < count or count % size:
        size += 1
    return size


def lane_norms(points):
    squares = jnp.square(points.astype(jnp.float32))
    high = squares.astype(jnp.bfloat16)
    low = (squares - high.astype(jnp.float32)).astype(jnp.bfloat16)
    ones = jnp.ones((8, points.shape[1]), jnp.bfloat16)
    dims = (((1,), (1,)), ((), ()))
    return lax.dot_general(
        ones, high, dims, preferred_element_type=jnp.float32
    ) + lax.dot_general(ones, low, dims, preferred_element_type=jnp.float32)


def fold8(array):
    return jnp.sum(array.reshape(array.shape[0] // 8, 8, array.shape[1]), 0)


def stack8(arrays):
    row = lax.broadcasted_iota(jnp.int32, (8, LANES), 0)
    for shift in (1, 2, 4):
        even = (row & shift) == 0
        arrays = [
            jnp.where(even, a, b) + pltpu.roll(jnp.where(even, b, a), shift, 0)
            for a, b in zip(arrays[::2], arrays[1::2])
        ]
    return arrays[0]


def powers(widest):
    middle = widest * widest
    return [middle * middle, middle, widest]


def kernel(
    plane,
    depth,
    x_hbm,
    y_hbm,
    out,
    rows,
    cols,
    parts,
    tots,
    load_sem,
    row_send,
    row_recv,
    col_send,
    col_recv,
    part_send,
    part_recv,
    tot_send,
    tot_recv,
):
    length, dim = x_hbm.shape
    count = plane * depth * length
    tiles = plane * length // LANES
    chunks = depth * length // LANES
    per_tile = LANES // length
    me = lax.axis_index("blk")
    mine = lax.rem(me, plane)
    layer = me // plane

    loads = [
        pltpu.make_async_copy(source, buffer.at[slot, pl.ds(first, length)], load_sem.at[k])
        for k, (source, buffer, slot, first) in enumerate(
            [
                (x_hbm, rows, mine, 0),
                (y_hbm, rows, mine, length),
                (x_hbm, cols, layer, 0),
                (y_hbm, cols, layer, length),
            ]
        )
    ]
    for load in loads:
        load.start()

    plane_peers = [layer * plane + lax.rem(mine + k, plane) for k in range(1, plane)]
    depth_peers = [lax.rem(layer + k, depth) * plane + mine for k in range(1, depth)]

    barrier = pltpu.get_barrier_semaphore()
    for peer in depth_peers + plane_peers:
        pl.semaphore_signal(barrier, inc=1, device_id=(peer,), device_id_type=MESH)
    for load in loads:
        load.wait()
    pl.semaphore_wait(barrier, plane + depth - 2)

    def spread(buffer, slot, peers, send, recv):
        copies = []
        for k, peer in enumerate(peers):
            copy = pltpu.make_async_remote_copy(
                src_ref=buffer.at[slot],
                dst_ref=buffer.at[slot],
                send_sem=send.at[k],
                recv_sem=recv.at[k],
                device_id=(peer,),
                device_id_type=MESH,
            )
            copy.start()
            copies.append(copy)
        return copies

    col_copies = spread(cols, layer, depth_peers, col_send, col_recv)
    row_copies = spread(rows, mine, plane_peers, row_send, row_recv)
    for copy in row_copies:
        copy.wait_recv()
    for copy in col_copies:
        copy.wait_recv()

    scale = -math.log2(math.e) / (2.0 * WIDTHS[2] * dim)
    dims = (((1,), (1,)), ((), ()))

    def tile_sums(tile):
        blocks = pl.ds(tile * per_tile, per_tile)
        left_x = rows[blocks, :length].reshape(LANES, dim)
        left_y = rows[blocks, length:].reshape(LANES, dim)
        left = jnp.concatenate([left_x, left_y], 0)
        norms = lane_norms(left)
        left_sq_x, left_sq_y = norms[:1, :LANES], norms[:1, LANES:]
        row_index = (
            layer * (plane * length)
            + tile * LANES
            + lax.broadcasted_iota(jnp.int32, (STEP, LANES), 1)
        )

        def chunk_sums(chunk, sums):
            blocks = pl.ds(chunk * per_tile, per_tile)
            right_x = cols[blocks, :length].reshape(LANES, dim)
            right_y = cols[blocks, length:].reshape(LANES, dim)
            right = jnp.concatenate([right_x, right_y], 0)
            right_sq = jnp.sum(jnp.square(right.astype(jnp.float32)), 1, keepdims=True)
            products = lax.dot_general(
                right * jnp.bfloat16(-2.0), left, dims, preferred_element_type=jnp.float32
            )
            sums = list(sums)
            for first in range(0, LANES, STEP):
                inner = lax.broadcasted_iota(jnp.int32, (STEP, LANES), 0)
                col_index = (
                    (chunk * per_tile + first // length) * plane + mine
                ) * length + (inner + first % length)
                diagonal = row_index == col_index
                sq_x = right_sq[first : first + STEP]
                sq_y = right_sq[LANES + first : LANES + first + STEP]

                def widest(left_sq, right_sq, products):
                    distance = jnp.maximum(left_sq + right_sq + products, 0.0)
                    return jnp.exp2(distance * scale)

                top = products[first : first + STEP]
                bottom = products[LANES + first : LANES + first + STEP]
                same_x = widest(left_sq_x, sq_x, top[:, :LANES])
                same_y = widest(left_sq_y, sq_y, bottom[:, LANES:])
                cross_xy = widest(left_sq_x, sq_y, bottom[:, :LANES])
                cross_yx = widest(left_sq_y, sq_x, top[:, LANES:])
                hadamard = same_x * same_y
                same_x = jnp.where(diagonal, 0.0, same_x)
                same_y = jnp.where(diagonal, 0.0, same_y)
                terms = []
                for value in (same_x, same_y, hadamard, cross_xy, cross_yx):
                    terms += powers(value)
                sums = [a + fold8(b) for a, b in zip(sums, terms)]
            return tuple(sums)

        sums = tuple(jnp.zeros((8, LANES), jnp.float32) for _ in range(15))
        if chunks == 1:
            sums = chunk_sums(0, sums)
        else:
            sums = lax.fori_loop(0, chunks, chunk_sums, sums)
        order = [0, 1, 2, 3, 4, 5, 6, 7, 9, 10, 11, 12, 13, 14, 8]
        flat = [sums[k] for k in order] + [jnp.zeros((8, LANES), jnp.float32)]
        parts[mine, tile, :8] = stack8(flat[:8])
        parts[mine, tile, 8:] = stack8(flat[8:])

    if tiles <= 2:
        for tile in range(tiles):
            tile_sums(tile)
    else:

        @pl.loop(0, tiles)
        def _(tile):
            tile_sums(tile)

    part_copies = spread(parts, mine, plane_peers, part_send, part_recv)
    for copy in part_copies:
        copy.wait_recv()

    def whole_sums(tile):
        total = parts[0, tile]
        for k in range(1, plane):
            total = total + parts[k, tile]
        return total[:8], total[8:]

    upper_total = jnp.zeros((8, LANES), jnp.float32)
    lower_total = jnp.zeros((8, LANES), jnp.float32)
    cross_total = jnp.zeros((8, LANES), jnp.float32)
    for tile in range(tiles):
        upper, lower = whole_sums(tile)
        upper_total += upper
        lower_total += lower
        cross_total += (upper + 1.0) * (pltpu.roll(upper, 5, 0) + 1.0)
    row = lax.broadcasted_iota(jnp.int32, (8, LANES), 0)
    lane = lax.broadcasted_iota(jnp.int32, (8, LANES), 1)

    def along_lanes(array):
        sums = jnp.where(row == lane, jnp.sum(array, 1, keepdims=True), 0.0)
        return jnp.broadcast_to(jnp.sum(sums, 0, keepdims=True), (8, LANES))

    upper = along_lanes(upper_total)
    lower = along_lanes(lower_total)
    cross = along_lanes(cross_total)
    paired = pltpu.roll(upper, LANES - 3, 1)
    hadamard = jnp.where(
        lane < 2, pltpu.roll(upper, LANES - 6, 1), pltpu.roll(lower, LANES - 4, 1)
    )
    size = float(count)
    mmd = (upper + paired) * (1.0 / (size - 1.0)) - lower * (2.0 / size)
    hsic = hadamard * (1.0 / size) - cross * (2.0 / (size * size))
    tots[layer] = jnp.where(
        row == 0, mmd, jnp.where(row == 1, hsic, jnp.where(row == 2, upper, paired))
    )
    tot_copies = spread(tots, layer, depth_peers, tot_send, tot_recv)

    upper, lower = whole_sums(mine // per_tile)
    scores = jnp.log(upper) - jnp.log(lower)
    turn = lax.rem(LANES - lax.rem(mine, per_tile) * length, LANES)
    scores = pltpu.roll(scores, turn, 1)

    for copy in tot_copies:
        copy.wait_recv()
    total = tots[0]
    for k in range(1, depth):
        total = total + tots[k]
    means = total * (1.0 / size) + 1.0
    product = means[2:3] * means[3:4] * (1.0 / size)
    out[...] = jnp.where(
        row < 6, scores, jnp.where(row == 6, total[0:1], total[1:2] + product)
    )
    for copy in col_copies + row_copies + part_copies + tot_copies:
        copy.wait_send()


def unpack(packed, x_out, y_out, mmd_out, hsic_out):
    length = x_out.shape[1]
    x_out[...] = packed[0:3, :length]
    y_out[...] = packed[3:6, :length]
    mmd_out[...] = packed[6:7, :3]
    hsic_out[...] = packed[7:8, :3]


def shards(x_points, y_points):
    length, dim = x_points.shape
    count = lax.axis_size("blk")
    plane = plane_size(count)
    depth = count // plane
    tiles = plane * length // LANES
    dma = pltpu.SemaphoreType.DMA
    packed = pl.pallas_call(
        functools.partial(kernel, plane, depth),
        out_shape=jax.ShapeDtypeStruct((8, LANES), jnp.float32),
        in_specs=[pl.BlockSpec(memory_space=pl.ANY)] * 2,
        out_specs=pl.BlockSpec(memory_space=pltpu.VMEM),
        scratch_shapes=[
            pltpu.VMEM((plane, 2 * length, dim), jnp.bfloat16),
            pltpu.VMEM((depth, 2 * length, dim), jnp.bfloat16),
            pltpu.VMEM((plane, tiles, 16, LANES), jnp.float32),
            pltpu.VMEM((depth, 8, LANES), jnp.float32),
            dma((4,)),
            dma((plane,)),
            dma((plane,)),
            dma((depth,)),
            dma((depth,)),
            dma((plane,)),
            dma((plane,)),
            dma((depth,)),
            dma((depth,)),
        ],
        compiler_params=pltpu.CompilerParams(collective_id=0, has_side_effects=True),
    )(x_points, y_points)
    x_scores, y_scores, mmd, hsic = pl.pallas_call(
        unpack,
        out_shape=(
            jax.ShapeDtypeStruct((3, length), jnp.float32),
            jax.ShapeDtypeStruct((3, length), jnp.float32),
            jax.ShapeDtypeStruct((1, 3), jnp.float32),
            jax.ShapeDtypeStruct((1, 3), jnp.float32),
        ),
    )(packed)
    return x_scores.T, y_scores.T, mmd[0], hsic[0]


def solution(mesh):
    placed = (P("blk", None), P("blk", None))
    return jax.shard_map(
        shards,
        mesh=mesh,
        in_specs=placed,
        out_specs=(P("blk", None), P("blk", None), P(), P()),
        check_vma=False,
    )
```

```python
import functools
import math

import jax
import jax.numpy as jnp
from jax import lax
from jax.experimental import pallas as pl
from jax.experimental.pallas import tpu as pltpu
from jax.sharding import PartitionSpec as P

WIDTHS = (0.08, 0.16, 0.32)
LANES = 128
STEP = 16
MESH = pl.DeviceIdType.MESH


def plane_size(count):
    size = math.isqrt(count)
    while size * size < count or count % size:
        size += 1
    return size


def others(index, size):
    if size & (size - 1):
        return [lax.rem(index + k, size) for k in range(1, size)]
    found = []
    for k in range(size - 1, 0, -1):
        other, bit = index, 1
        while bit < size:
            if k & bit:
                other = other + bit - 2 * bit * lax.rem(index // bit, 2)
            bit *= 2
        found.append(other)
    return found


def lane_norms(points):
    squares = jnp.square(points.astype(jnp.float32))
    high = squares.astype(jnp.bfloat16)
    low = (squares - high.astype(jnp.float32)).astype(jnp.bfloat16)
    ones = jnp.ones((8, points.shape[1]), jnp.bfloat16)
    dims = (((1,), (1,)), ((), ()))
    return lax.dot_general(
        ones, high, dims, preferred_element_type=jnp.float32
    ) + lax.dot_general(ones, low, dims, preferred_element_type=jnp.float32)


def fold8(array):
    return jnp.sum(array.reshape(array.shape[0] // 8, 8, array.shape[1]), 0)


def stack8(arrays):
    row = lax.broadcasted_iota(jnp.int32, (8, LANES), 0)
    for shift in (1, 2, 4):
        even = (row & shift) == 0
        arrays = [
            jnp.where(even, a, b) + pltpu.roll(jnp.where(even, b, a), shift, 0)
            for a, b in zip(arrays[::2], arrays[1::2])
        ]
    return arrays[0]


def powers(widest):
    middle = widest * widest
    return [middle * middle, middle, widest]


def kernel(
    plane,
    depth,
    x_hbm,
    y_hbm,
    out,
    rows,
    cols,
    parts,
    tots,
    load_sem,
    row_send,
    row_recv,
    col_send,
    col_recv,
    part_send,
    part_recv,
    tot_send,
    tot_recv,
):
    length, dim = x_hbm.shape
    count = plane * depth * length
    tiles = depth * length // LANES
    chunks = plane * length // LANES
    per_tile = LANES // length
    me = lax.axis_index("blk")
    mine = lax.rem(me, plane)
    layer = me // plane

    loads = [
        pltpu.make_async_copy(source, buffer.at[slot, pl.ds(first, length)], load_sem.at[k])
        for k, (source, buffer, slot, first) in enumerate(
            [
                (x_hbm, rows, layer, 0),
                (y_hbm, rows, layer, length),
                (x_hbm, cols, mine, 0),
                (y_hbm, cols, mine, length),
            ]
        )
    ]
    for load in loads:
        load.start()

    plane_peers = [layer * plane + other for other in others(mine, plane)]
    depth_peers = [other * plane + mine for other in others(layer, depth)]

    barrier = pltpu.get_barrier_semaphore()
    for peer in depth_peers + plane_peers:
        pl.semaphore_signal(barrier, inc=1, device_id=(peer,), device_id_type=MESH)
    for load in loads:
        load.wait()
    pl.semaphore_wait(barrier, plane + depth - 2)

    def spread(buffer, slot, peers, send, recv):
        copies = []
        for k, peer in enumerate(peers):
            copy = pltpu.make_async_remote_copy(
                src_ref=buffer.at[slot],
                dst_ref=buffer.at[slot],
                send_sem=send.at[k],
                recv_sem=recv.at[k],
                device_id=(peer,),
                device_id_type=MESH,
            )
            copy.start()
            copies.append(copy)
        return copies

    row_copies = spread(rows, layer, depth_peers, row_send, row_recv)
    col_copies = spread(cols, mine, plane_peers, col_send, col_recv)
    for copy in col_copies:
        copy.wait_recv()
    for copy in row_copies:
        copy.wait_recv()

    scale = -math.log2(math.e) / (2.0 * WIDTHS[2] * dim)
    dims = (((1,), (1,)), ((), ()))

    def tile_sums(tile):
        blocks = pl.ds(tile * per_tile, per_tile)
        left_x = rows[blocks, :length].reshape(LANES, dim)
        left_y = rows[blocks, length:].reshape(LANES, dim)
        left = jnp.concatenate([left_x, left_y], 0)
        norms = lane_norms(left)
        left_sq_x, left_sq_y = norms[:1, :LANES], norms[:1, LANES:]
        lane = lax.broadcasted_iota(jnp.int32, (STEP, LANES), 1)
        row_index = (
            (tile * per_tile + lane // length) * plane + mine
        ) * length + lax.rem(lane, length)

        def chunk_sums(chunk, sums):
            blocks = pl.ds(chunk * per_tile, per_tile)
            right_x = cols[blocks, :length].reshape(LANES, dim)
            right_y = cols[blocks, length:].reshape(LANES, dim)
            right = jnp.concatenate([right_x, right_y], 0)
            right_sq = jnp.sum(jnp.square(right.astype(jnp.float32)), 1, keepdims=True)
            products = lax.dot_general(
                right * jnp.bfloat16(-2.0), left, dims, preferred_element_type=jnp.float32
            )
            sums = list(sums)
            for first in range(0, LANES, STEP):
                inner = lax.broadcasted_iota(jnp.int32, (STEP, LANES), 0)
                col_index = layer * (plane * length) + chunk * LANES + first + inner
                diagonal = row_index == col_index
                sq_x = right_sq[first : first + STEP]
                sq_y = right_sq[LANES + first : LANES + first + STEP]

                def widest(left_sq, right_sq, products):
                    distance = jnp.maximum(left_sq + right_sq + products, 0.0)
                    return jnp.exp2(distance * scale)

                top = products[first : first + STEP]
                bottom = products[LANES + first : LANES + first + STEP]
                same_x = widest(left_sq_x, sq_x, top[:, :LANES])
                same_y = widest(left_sq_y, sq_y, bottom[:, LANES:])
                cross_xy = widest(left_sq_x, sq_y, bottom[:, :LANES])
                cross_yx = widest(left_sq_y, sq_x, top[:, LANES:])
                hadamard = same_x * same_y
                same_x = jnp.where(diagonal, 0.0, same_x)
                same_y = jnp.where(diagonal, 0.0, same_y)
                terms = []
                for value in (same_x, same_y, hadamard, cross_xy, cross_yx):
                    terms += powers(value)
                sums = [a + fold8(b) for a, b in zip(sums, terms)]
            return tuple(sums)

        sums = tuple(jnp.zeros((8, LANES), jnp.float32) for _ in range(15))
        if chunks <= 2:
            for chunk in range(chunks):
                sums = chunk_sums(chunk, sums)
        else:
            sums = lax.fori_loop(0, chunks, chunk_sums, sums)
        order = [0, 1, 2, 3, 4, 5, 6, 7, 9, 10, 11, 12, 13, 14, 8]
        flat = [sums[k] for k in order] + [jnp.zeros((8, LANES), jnp.float32)]
        parts[layer, tile, :8] = stack8(flat[:8])
        parts[layer, tile, 8:] = stack8(flat[8:])

    if tiles <= 2:
        for tile in range(tiles):
            tile_sums(tile)
    else:

        @pl.loop(0, tiles)
        def _(tile):
            tile_sums(tile)

    part_copies = spread(parts, layer, depth_peers, part_send, part_recv)
    for copy in part_copies:
        copy.wait_recv()

    def whole_sums(tile):
        total = parts[0, tile]
        for k in range(1, depth):
            total = total + parts[k, tile]
        return total[:8], total[8:]

    upper_total = jnp.zeros((8, LANES), jnp.float32)
    lower_total = jnp.zeros((8, LANES), jnp.float32)
    cross_total = jnp.zeros((8, LANES), jnp.float32)
    for tile in range(tiles):
        upper, lower = whole_sums(tile)
        upper_total += upper
        lower_total += lower
        cross_total += (upper + 1.0) * (pltpu.roll(upper, 5, 0) + 1.0)
    row = lax.broadcasted_iota(jnp.int32, (8, LANES), 0)
    lane = lax.broadcasted_iota(jnp.int32, (8, LANES), 1)

    def along_lanes(array):
        sums = jnp.where(row == lane, jnp.sum(array, 1, keepdims=True), 0.0)
        return jnp.broadcast_to(jnp.sum(sums, 0, keepdims=True), (8, LANES))

    upper = along_lanes(upper_total)
    lower = along_lanes(lower_total)
    cross = along_lanes(cross_total)
    paired = pltpu.roll(upper, LANES - 3, 1)
    hadamard = jnp.where(
        lane < 2, pltpu.roll(upper, LANES - 6, 1), pltpu.roll(lower, LANES - 4, 1)
    )
    size = float(count)
    mmd = (upper + paired) * (1.0 / (size - 1.0)) - lower * (2.0 / size)
    hsic = hadamard * (1.0 / size) - cross * (2.0 / (size * size))
    tots[mine] = jnp.where(
        row == 0, mmd, jnp.where(row == 1, hsic, jnp.where(row == 2, upper, paired))
    )
    tot_copies = spread(tots, mine, plane_peers, tot_send, tot_recv)

    upper, lower = whole_sums(layer // per_tile)
    scores = jnp.log(upper) - jnp.log(lower)
    turn = lax.rem(LANES - lax.rem(layer, per_tile) * length, LANES)
    scores = pltpu.roll(scores, turn, 1)

    for copy in tot_copies:
        copy.wait_recv()
    total = tots[0]
    for k in range(1, plane):
        total = total + tots[k]
    means = total * (1.0 / size) + 1.0
    product = means[2:3] * means[3:4] * (1.0 / size)
    out[...] = jnp.where(
        row < 6, scores, jnp.where(row == 6, total[0:1], total[1:2] + product)
    )
    for copy in col_copies + row_copies + part_copies + tot_copies:
        copy.wait_send()


def unpack(packed, x_out, y_out, mmd_out, hsic_out):
    length = x_out.shape[1]
    x_out[...] = packed[0:3, :length]
    y_out[...] = packed[3:6, :length]
    mmd_out[...] = packed[6:7, :3]
    hsic_out[...] = packed[7:8, :3]


def shards(x_points, y_points):
    length, dim = x_points.shape
    count = lax.axis_size("blk")
    plane = plane_size(count)
    depth = count // plane
    tiles = depth * length // LANES
    dma = pltpu.SemaphoreType.DMA
    packed = pl.pallas_call(
        functools.partial(kernel, plane, depth),
        out_shape=pltpu.VMEM((8, LANES), jnp.float32),
        in_specs=[pl.BlockSpec(memory_space=pl.ANY)] * 2,
        out_specs=pl.BlockSpec(memory_space=pltpu.VMEM),
        scratch_shapes=[
            pltpu.VMEM((depth, 2 * length, dim), jnp.bfloat16),
            pltpu.VMEM((plane, 2 * length, dim), jnp.bfloat16),
            pltpu.VMEM((depth, tiles, 16, LANES), jnp.float32),
            pltpu.VMEM((plane, 8, LANES), jnp.float32),
            dma((4,)),
            dma((depth,)),
            dma((depth,)),
            dma((plane,)),
            dma((plane,)),
            dma((depth,)),
            dma((depth,)),
            dma((plane,)),
            dma((plane,)),
        ],
        compiler_params=pltpu.CompilerParams(collective_id=0, has_side_effects=True),
    )(x_points, y_points)
    x_scores, y_scores, mmd, hsic = pl.pallas_call(
        unpack,
        in_specs=[pl.BlockSpec(memory_space=pltpu.VMEM)],
        out_shape=(
            jax.ShapeDtypeStruct((3, length), jnp.float32),
            jax.ShapeDtypeStruct((3, length), jnp.float32),
            jax.ShapeDtypeStruct((1, 3), jnp.float32),
            jax.ShapeDtypeStruct((1, 3), jnp.float32),
        ),
    )(pltpu.with_memory_space_constraint(packed, pltpu.VMEM))
    return x_scores.T, y_scores.T, mmd[0], hsic[0]


def solution(mesh):
    placed = (P("blk", None), P("blk", None))
    return jax.shard_map(
        shards,
        mesh=mesh,
        in_specs=placed,
        out_specs=(P("blk", None), P("blk", None), P(), P()),
        check_vma=False,
    )
```
